128 devices in a mesh: tm: 16 (over z, x), pair: 8 (over y, core).
Axes of the slice: x: 4, y: 4, z: 4, core: 2. Of those that a mesh axis runs over, the one named last changes fastest.
Arguments:
- signal: float32 [2, 262144], P(None, 'tm'), may hold values from -6 to 6
- hop_offsets: int32 [4096], P(('tm', 'pair')), may hold values from 0 to 262143, as said below
- pair_channels: int32 [2, 16384], P(None, 'pair'), may hold values from 0 to 255
Outputs:
- surface: float32 [64, 16384], P(None, 'pair')
The draws below stay inside these ranges and needn't reach their ends.
Inputs may be any that keep to these rules, and one draw needn't show every extreme that they name: `hop_offsets`: hop p starts at a sample in p * 64 to p * 64 + 63.
All inputs are finite; a program needn't handle non-finite values.
Results may differ from the reference program's by a relative error of at most 0.000071.
Values sent between devices are 32-bit elements; how exact they have to be, the bound alone decides.
A program may use at most 64 MiB of HBM per device.

```python
import math
import jax
import jax.numpy as jnp
from jax import lax

NP = 256
Q = 64
STRIDE = 64
HOPS = 4096
SAMPLES = 262144
PAIRS = 16384
NBLK = 64


def draw_hop_offsets(key, part):
    jitter = jax.random.randint(jax.random.fold_in(key, 11), (HOPS,), 0, STRIDE, dtype=jnp.int32)
    return jnp.arange(HOPS, dtype=jnp.int32) * STRIDE + jitter


def with_ends(values, stream_key, smallest, largest):
    shape = values.shape
    spot = [jax.random.randint(jax.random.fold_in(stream_key, axis), (), 0, shape[axis]) for axis in range(len(shape))]
    values = values.at[tuple(spot)].set(smallest)
    longest = shape.index(max(shape))
    spot[longest] = (spot[longest] + 1) % shape[longest]
    return values.at[tuple(spot)].set(largest)


def level_of(rng, dims, pieces, least, high):
    factor_of = 1.0
    for dim, blocks in pieces:
        draws = jax.random.uniform(jax.random.fold_in(jax.random.fold_in(rng, 6), dim), (blocks,), jnp.float32, least / len(pieces), high / len(pieces))
        factor_of = factor_of * jnp.repeat(jnp.exp(draws), dims[dim] // blocks).reshape((-1,) + (1,) * (len(dims) - 1 - dim))
    return factor_of


def centred(key, shape, deviation, most, split=(), held_as=jnp.bfloat16):
    array = deviation * jax.random.normal(key, shape, jnp.float32)
    if split:
        array = array * level_of(key, shape, split, -0.22, 0.18)
    return jnp.clip(array, -most, most).astype(held_as)


def setup_inputs(seed: int = 0) -> dict:
    splits = jax.random.split(jax.random.key(seed), 4)
    return {
        "signal": centred(splits[0], (2, SAMPLES), 1.0, 6.0, ((1, 16),), jnp.float32),
        "hop_offsets": draw_hop_offsets(jax.random.fold_in(splits[3], 71), 0),
        "pair_channels": with_ends(jax.random.randint(splits[2], (2, PAIRS), 0, NP), jax.random.fold_in(splits[2], 1), 0, NP - 1).astype(jnp.int32),
    }


def reference(signal, hop_offsets, pair_channels):
    extended = jnp.concatenate([signal, jnp.zeros((2, NP), signal.dtype)], axis=1)
    sample = jnp.arange(NP, dtype=jnp.int32)
    window = 0.54 - 0.46 * jnp.cos(2.0 * jnp.pi * sample.astype(signal.dtype) / NP)
    gainval = 1.0 / jnp.sqrt(jnp.sum(window * window))
    spots = hop_offsets[:, None] + sample[None, :]
    frames = (extended[0][spots] + 1j * extended[1][spots]) * window[None, :]
    spectra = jnp.fft.fft(frames, axis=1) * gainval
    turns = sample[None, :] * (hop_offsets[:, None] % NP) % NP
    theta = 2.0 * jnp.pi * turns.astype(signal.dtype) / NP
    spectra = spectra * jnp.exp(-1j * theta)
    width = math.gcd(PAIRS, 1024)
    grouped = pair_channels.reshape(2, PAIRS // width, width).transpose(1, 0, 2)

    def block_power(index):
        first = spectra[:, index[0]]
        second = spectra[:, index[1]]
        products = (first * jnp.conj(second)).reshape(NBLK, Q, width)
        cyclic = jnp.fft.fft(products, axis=1) / math.sqrt(Q)
        return lax.optimization_barrier(jnp.sum(jnp.real(cyclic) ** 2 + jnp.imag(cyclic) ** 2, axis=0))
    powers = lax.map(block_power, grouped)
    return powers.transpose(1, 0, 2).reshape(Q, PAIRS) / NBLK
```

```python
import numpy as np

import jax
import jax.numpy as jnp
from jax import lax
from jax.experimental import pallas as pl
from jax.experimental.pallas import tpu as pltpu
from jax.sharding import PartitionSpec as P

NP = 256
Q = 64
TM = 16
PAIR = 8
HOPS = 256
PAIRS = 2048
WIDTH = 256
CHUNKS = PAIRS // WIDTH
SLICE = PAIRS // TM
BLOCKS = HOPS // Q
MESH = pl.DeviceIdType.MESH
F32 = jnp.float32
BF16 = jnp.bfloat16


def split(table):
    high = table.astype(np.float32).astype(BF16)
    low = (table - high.astype(np.float64)).astype(np.float32).astype(BF16)
    return high, low


def tables():
    sample = np.arange(NP // 2)
    out = []
    for odd in (0, 1):
        turns = np.outer(sample, 2 * sample + odd) % NP
        angle = 2.0 * np.pi * turns / NP
        cosine, sine = np.cos(angle), np.sin(angle)
        table = np.block([[cosine, -sine], [sine, cosine]])
        out.extend(split(table))
    hop = (4 * np.arange(Q // 4)[None, :] + np.arange(4)[:, None]).reshape(Q)
    turns = np.outer(np.arange(Q), hop) % Q
    angle = 2.0 * np.pi * turns / Q
    cosine, sine = np.cos(angle) / 8.0, np.sin(angle) / 8.0
    high, low = split(np.block([[cosine, sine], [-sine, cosine]]))
    upper = np.concatenate([high, high], axis=1)
    lower = np.concatenate([low, np.zeros_like(low)], axis=1)
    out.append(np.concatenate([upper, lower], axis=0))
    return np.stack(out)


def window_rows():
    sample = np.arange(NP)
    angle = 2.0 * np.pi * sample / NP
    window = 0.54 - 0.46 * np.cos(angle)
    gain = 1.0 / np.sqrt(np.sum(window * window))
    rows = np.zeros((8, NP))
    rows[0] = 0.54 * gain
    rows[1] = -0.46 * gain * np.cos(angle)
    rows[2] = -0.46 * gain * np.sin(angle)
    return rows.astype(np.float32)


def high_low(value):
    high = value.astype(BF16)
    return high, (value - high.astype(F32)).astype(BF16)


def dot(left, right):
    return jnp.dot(left, right, preferred_element_type=F32)


def kernel(
    sig_ref, off_ref, pc_ref, win_ref, tab_hbm, out_ref,
    rows_ref, edge_ref, msg_ref, tab_ref, grid_ref, spec_ref, hot_ref,
    part_ref, recv_ref, done_ref,
    tab_sem, edge_send, edge_recv, msg_send, msg_recv, part_send, part_recv, done_send, done_recv,
):
    tm = lax.axis_index("tm")
    pr = lax.axis_index("pair")

    barrier = pltpu.get_barrier_semaphore()

    def greet_tm(step, carry):
        peer = lax.rem(tm + step, TM)
        pl.semaphore_signal(barrier, inc=1, device_id=(peer, pr), device_id_type=MESH)
        return carry

    def greet_pair(step, carry):
        peer = lax.rem(pr + step, PAIR)
        pl.semaphore_signal(barrier, inc=1, device_id=(tm, peer), device_id_type=MESH)
        return carry

    lax.fori_loop(1, TM, greet_tm, 0)
    lax.fori_loop(1, PAIR, greet_pair, 0)

    tab_copy = pltpu.make_async_copy(tab_hbm, tab_ref, tab_sem)
    tab_copy.start()

    lane = lax.broadcasted_iota(jnp.int32, (8, 128), 1)
    row32 = lax.broadcasted_iota(jnp.int32, (8, 32), 0)
    lane32 = lax.broadcasted_iota(jnp.int32, (8, 32), 1)
    shift = (off_ref[...] & (NP - 1)).astype(F32)
    shift = jnp.broadcast_to(shift, (8, 32))
    value = jnp.zeros((8, 128), F32)
    for u in range(4):
        column = jnp.sum(jnp.where(lane32 == 4 * row32 + u, shift, 0.0), axis=1, keepdims=True)
        value = jnp.where((lane & 3) == u, column, value)
    theta = value * (2.0 * np.pi / NP)
    value = jnp.where(lane < 4, value, jnp.where(lane < 8, jnp.cos(theta), jnp.sin(theta)))
    msg_ref[pr] = value

    for group in range(HOPS // 2):
        rows_ref[2 * group : 2 * group + 2, :] = sig_ref[:, 128 * group : 128 * (group + 1)]

    pl.semaphore_wait(barrier, TM + PAIR - 2)

    def edge_copy():
        return pltpu.make_async_remote_copy(
            src_ref=sig_ref.at[:, pl.ds(0, NP)],
            dst_ref=edge_ref,
            send_sem=edge_send,
            recv_sem=edge_recv,
            device_id=(lax.rem(tm + TM - 1, TM), pr),
            device_id_type=MESH,
        )

    def msg_copy(slot, peer):
        return pltpu.make_async_remote_copy(
            src_ref=msg_ref.at[slot],
            dst_ref=msg_ref.at[slot],
            send_sem=msg_send.at[peer],
            recv_sem=msg_recv.at[slot],
            device_id=(tm, peer),
            device_id_type=MESH,
        )

    edge_copy().start()

    def send_msg(step, carry):
        msg_copy(pr, lax.rem(pr + step, PAIR)).start()
        return carry

    lax.fori_loop(1, PAIR, send_msg, 0)

    channel = lax.broadcasted_iota(jnp.int32, (NP, WIDTH), 0)

    def build_hot(chunk, carry):
        start = pl.multiple_of(chunk * WIDTH, WIDTH)
        for side in range(2):
            index = pc_ref[side : side + 1, pl.ds(start, WIDTH)]
            index = (index >> 1) + (index & 1) * (NP // 2)
            hot_ref[chunk, side] = jnp.where(channel == index, 1.0, 0.0).astype(BF16)
        return carry

    lax.fori_loop(0, CHUNKS, build_hot, 0)
    tab_copy.wait()

    edge_copy().wait_recv()

    def wait_msg(step, carry):
        slot = lax.rem(pr + step, PAIR)
        msg_copy(slot, slot).wait_recv()
        return carry

    lax.fori_loop(1, PAIR, wait_msg, 0)

    last = tm == TM - 1
    edge = jnp.where(last, 0.0, edge_ref[...])
    rows_ref[HOPS : HOPS + 2, :] = edge[:, :128]
    rows_ref[HOPS + 2 : HOPS + 4, :] = edge[:, 128:]

    messages = msg_ref[...].reshape(Q, 128)
    column = lax.broadcasted_iota(jnp.int32, (Q, 128), 1).astype(F32)

    def samples(part, half, ahead):
        return rows_ref[pl.ds(2 * half + part + 4 * ahead, Q, stride=4), :]

    for u in range(4):
        start = messages[:, u : u + 1]
        cosine = messages[:, 4 + u : 5 + u]
        sine = messages[:, 8 + u : 9 + u]
        halves = []
        for half in range(2):
            lanes = slice(128 * half, 128 * half + 128)
            weight = win_ref[0:1, lanes] + cosine * win_ref[1:2, lanes] + sine * win_ref[2:3, lanes]
            here = column + 128.0 * half >= start
            halves.append(
                [jnp.where(here, samples(part, half, 0), samples(part, half, 1)) * weight for part in range(2)]
            )
        for sign in range(2):
            for part in range(2):
                left, right = halves[0][part], halves[1][part]
                high, low = high_low(left - right if sign else left + right)
                grid_ref[sign, 0, u * Q : (u + 1) * Q, 128 * part : 128 * (part + 1)] = high
                grid_ref[sign, 1, u * Q : (u + 1) * Q, 128 * part : 128 * (part + 1)] = low

    for odd in range(2):
        high, low = grid_ref[odd, 0], grid_ref[odd, 1]
        result = dot(high, tab_ref[2 * odd]) + dot(low, tab_ref[2 * odd]) + dot(high, tab_ref[2 * odd + 1])
        high, low = high_low(result)
        for u in range(4):
            for block in range(BLOCKS):
                source = slice(u * Q + 16 * block, u * Q + 16 * block + 16)
                for part in range(2):
                    target = slice(block * 128 + part * 64 + 16 * u, block * 128 + part * 64 + 16 * u + 16)
                    lanes = slice(128 * part, 128 * part + 128)
                    spec_ref[target, 128 * odd : 128 * odd + 128] = high[source, lanes]
                    spec_ref[target, 256 + 128 * odd : 384 + 128 * odd] = low[source, lanes]

    def part_copy(slot, owner):
        return pltpu.make_async_remote_copy(
            src_ref=part_ref.at[owner],
            dst_ref=recv_ref.at[slot],
            send_sem=part_send.at[owner],
            recv_sem=part_recv.at[slot],
            device_id=(owner, pr),
            device_id_type=MESH,
        )

    def compute(step, carry):
        chunk = lax.rem(tm // 2 + 1 + step, CHUNKS)
        pick_a = hot_ref[chunk, 0]
        pick_b = hot_ref[chunk, 1]
        first = dot(spec_ref[:, :NP], pick_a) + dot(spec_ref[:, NP:], pick_a)
        second = dot(spec_ref[:, :NP], pick_b) + dot(spec_ref[:, NP:], pick_b)
        power = jnp.zeros((Q, WIDTH), F32)
        for block in range(BLOCKS):
            base = block * 2 * Q
            first_re, first_im = first[base : base + Q], first[base + Q : base + 2 * Q]
            second_re, second_im = second[base : base + Q], second[base + Q : base + 2 * Q]
            re_high, re_low = high_low(first_re * second_re + first_im * second_im)
            im_high, im_low = high_low(first_im * second_re - first_re * second_im)
            stacked = jnp.concatenate([re_high, im_high, re_low, im_low], axis=0)
            both = dot(tab_ref[4], stacked)
            cyclic = both[: 2 * Q] + both[2 * Q :]
            square = cyclic * cyclic
            power = power + square[:Q] + square[Q:]
        for half in range(2):
            owner = 2 * chunk + half
            part_ref[owner] = power[:, half * SLICE : (half + 1) * SLICE]

            @pl.when(owner != tm)
            def send():
                part_copy(tm, owner).start()

        return carry

    lax.fori_loop(0, CHUNKS, compute, 0)

    def absorb(step, total):
        slot = lax.rem(tm + step, TM)
        part_copy(slot, slot).wait_recv()
        return total + recv_ref[slot]

    total = lax.fori_loop(1, TM, absorb, part_ref[tm])
    done_ref[tm] = total * (1.0 / Q)

    def done_copy(slot, peer):
        return pltpu.make_async_remote_copy(
            src_ref=done_ref.at[slot],
            dst_ref=done_ref.at[slot],
            send_sem=done_send.at[peer],
            recv_sem=done_recv.at[slot],
            device_id=(peer, pr),
            device_id_type=MESH,
        )

    def send_done(step, carry):
        done_copy(tm, lax.rem(tm + step, TM)).start()
        return carry

    lax.fori_loop(1, TM, send_done, 0)

    def wait_done(step, carry):
        slot = lax.rem(tm + step, TM)
        done_copy(slot, slot).wait_recv()
        return carry

    lax.fori_loop(1, TM, wait_done, 0)
    for slot in range(TM):
        out_ref[:, SLICE * slot : SLICE * (slot + 1)] = done_ref[slot]

    edge_copy().wait_send()

    def drain_msg(step, carry):
        msg_copy(pr, lax.rem(pr + step, PAIR)).wait_send()
        return carry

    def drain_tm(step, carry):
        peer = lax.rem(tm + step, TM)
        part_copy(tm, peer).wait_send()
        done_copy(tm, peer).wait_send()
        return carry

    lax.fori_loop(1, PAIR, drain_msg, 0)
    lax.fori_loop(1, TM, drain_tm, 0)


def shards(signal, hop_offsets, pair_channels):
    vmem = pl.BlockSpec(memory_space=pltpu.VMEM)
    return pl.pallas_call(
        kernel,
        out_shape=jax.ShapeDtypeStruct((Q, PAIRS), F32),
        in_specs=[vmem, vmem, vmem, vmem, pl.BlockSpec(memory_space=pl.ANY)],
        out_specs=vmem,
        scratch_shapes=[
            pltpu.VMEM((HOPS + 8, 128), F32),
            pltpu.VMEM((2, NP), F32),
            pltpu.VMEM((PAIR, 8, 128), F32),
            pltpu.VMEM((5, NP, NP), BF16),
            pltpu.VMEM((2, 2, HOPS, NP), BF16),
            pltpu.VMEM((2 * HOPS, 2 * NP), BF16),
            pltpu.VMEM((CHUNKS, 2, NP, WIDTH), BF16),
            pltpu.VMEM((TM, Q, SLICE), F32),
            pltpu.VMEM((TM, Q, SLICE), F32),
            pltpu.VMEM((TM, Q, SLICE), F32),
            pltpu.SemaphoreType.DMA,
            pltpu.SemaphoreType.DMA,
            pltpu.SemaphoreType.DMA,
            pltpu.SemaphoreType.DMA((PAIR,)),
            pltpu.SemaphoreType.DMA((PAIR,)),
            pltpu.SemaphoreType.DMA((TM,)),
            pltpu.SemaphoreType.DMA((TM,)),
            pltpu.SemaphoreType.DMA((TM,)),
            pltpu.SemaphoreType.DMA((TM,)),
        ],
        compiler_params=pltpu.CompilerParams(
            collective_id=0, has_side_effects=True, vmem_limit_bytes=48 * 1024 * 1024
        ),
    )(
        signal,
        hop_offsets.reshape(1, HOPS // PAIR),
        pair_channels,
        jnp.asarray(window_rows()),
        jnp.asarray(tables()),
    )


def solution(mesh):
    return jax.shard_map(
        shards,
        mesh=mesh,
        in_specs=(P(None, "tm"), P(("tm", "pair")), P(None, "pair")),
        out_specs=P(None, "pair"),
        check_vma=False,
    )
```

```python
import numpy as np

import jax
import jax.numpy as jnp
from jax import lax
from jax.experimental import pallas as pl
from jax.experimental.pallas import tpu as pltpu
from jax.sharding import PartitionSpec as P

NP = 256
Q = 64
TM = 16
PAIR = 8
HOPS = 256
PAIRS = 2048
WIDTH = 256
CHUNKS = PAIRS // WIDTH
SLICE = PAIRS // TM
BLOCKS = HOPS // Q
MESH = pl.DeviceIdType.MESH
F32 = jnp.float32
BF16 = jnp.bfloat16


def split(table):
    high = table.astype(np.float32).astype(BF16)
    low = (table - high.astype(np.float64)).astype(np.float32).astype(BF16)
    return high, low


def tables():
    sample = np.arange(NP // 2)
    out = []
    for odd in (0, 1):
        turns = np.outer(sample, 2 * sample + odd) % NP
        angle = 2.0 * np.pi * turns / NP
        cosine, sine = np.cos(angle), np.sin(angle)
        table = np.block([[cosine, -sine], [sine, cosine]])
        out.extend(split(table))
    hop = (4 * np.arange(Q // 4)[None, :] + np.arange(4)[:, None]).reshape(Q)
    turns = np.outer(np.arange(Q), hop) % Q
    angle = 2.0 * np.pi * turns / Q
    cosine, sine = np.cos(angle) / 8.0, np.sin(angle) / 8.0
    high, low = split(np.block([[cosine, sine], [-sine, cosine]]))
    upper = np.concatenate([high, high], axis=1)
    lower = np.concatenate([low, np.zeros_like(low)], axis=1)
    out.append(np.concatenate([upper, lower], axis=0))
    return np.stack(out)


def window_rows():
    sample = np.arange(NP)
    angle = 2.0 * np.pi * sample / NP
    window = 0.54 - 0.46 * np.cos(angle)
    gain = 1.0 / np.sqrt(np.sum(window * window))
    rows = np.zeros((8, NP))
    rows[0] = 0.54 * gain
    rows[1] = -0.46 * gain * np.cos(angle)
    rows[2] = -0.46 * gain * np.sin(angle)
    return rows.astype(np.float32)


def high_low(value):
    high = value.astype(BF16)
    return high, (value - high.astype(F32)).astype(BF16)


def dot(left, right):
    return jnp.dot(left, right, preferred_element_type=F32)


def kernel(
    sig_hbm, off_hbm, pc_hbm, win_hbm, tab_hbm, out_ref,
    sig_ref, off_ref, pc_ref, win_ref, rows_ref, edge_ref, msg_ref, tab_ref, grid_ref, spec_ref, hot_ref,
    part_ref, recv_ref, done_ref,
    load_sem, edge_send, edge_recv, msg_send, msg_recv, part_send, part_recv, done_send, done_recv,
):
    tm = lax.axis_index("tm")
    pr = lax.axis_index("pair")

    with jax.named_scope("load_greet"):
        loads = [
            pltpu.make_async_copy(source, target, load_sem.at[index])
            for index, (source, target) in enumerate(
                (
                    (off_hbm, off_ref),
                    (sig_hbm, sig_ref),
                    (pc_hbm, pc_ref),
                    (win_hbm, win_ref),
                    (tab_hbm, tab_ref),
                )
            )
        ]
        for load in loads:
            load.start()
        barrier = pltpu.get_barrier_semaphore()

        def greet_tm(step, carry):
            peer = lax.rem(tm + step, TM)
            pl.semaphore_signal(barrier, inc=1, device_id=(peer, pr), device_id_type=MESH)
            return carry

        def greet_pair(step, carry):
            peer = lax.rem(pr + step, PAIR)
            pl.semaphore_signal(barrier, inc=1, device_id=(tm, peer), device_id_type=MESH)
            return carry

        lax.fori_loop(1, TM, greet_tm, 0)
        lax.fori_loop(1, PAIR, greet_pair, 0)

    with jax.named_scope("prep"):
        loads[0].wait()
        lane = lax.broadcasted_iota(jnp.int32, (8, 128), 1)
        row32 = lax.broadcasted_iota(jnp.int32, (8, 32), 0)
        lane32 = lax.broadcasted_iota(jnp.int32, (8, 32), 1)
        shift = (off_ref[...] & (NP - 1)).astype(F32)
        shift = jnp.broadcast_to(shift, (8, 32))
        value = jnp.zeros((8, 128), F32)
        for u in range(4):
            column = jnp.sum(jnp.where(lane32 == 4 * row32 + u, shift, 0.0), axis=1, keepdims=True)
            value = jnp.where((lane & 3) == u, column, value)
        theta = value * (2.0 * np.pi / NP)
        value = jnp.where(lane < 4, value, jnp.where(lane < 8, jnp.cos(theta), jnp.sin(theta)))
        msg_ref[pr] = value

        loads[1].wait()
        for group in range(HOPS // 2):
            rows_ref[2 * group : 2 * group + 2, :] = sig_ref[:, 128 * group : 128 * (group + 1)]

    with jax.named_scope("barrier"):
        pl.semaphore_wait(barrier, TM + PAIR - 2)

    with jax.named_scope("exchange_start"):
        def edge_copy():
            return pltpu.make_async_remote_copy(
                src_ref=sig_ref.at[:, pl.ds(0, NP)],
                dst_ref=edge_ref,
                send_sem=edge_send,
                recv_sem=edge_recv,
                device_id=(lax.rem(tm + TM - 1, TM), pr),
                device_id_type=MESH,
            )

        def msg_copy(slot, peer):
            return pltpu.make_async_remote_copy(
                src_ref=msg_ref.at[slot],
                dst_ref=msg_ref.at[slot],
                send_sem=msg_send.at[peer],
                recv_sem=msg_recv.at[slot],
                device_id=(tm, peer),
                device_id_type=MESH,
            )

        edge_copy().start()

        def send_msg(step, carry):
            msg_copy(pr, lax.rem(pr + step, PAIR)).start()
            return carry

        lax.fori_loop(1, PAIR, send_msg, 0)

    with jax.named_scope("hot"):
        channel = lax.broadcasted_iota(jnp.int32, (NP, WIDTH), 0)

        def build_hot(chunk, carry):
            start = pl.multiple_of(chunk * WIDTH, WIDTH)
            for side in range(2):
                index = pc_ref[side : side + 1, pl.ds(start, WIDTH)]
                index = (index >> 1) + (index & 1) * (NP // 2)
                hot_ref[chunk, side] = jnp.where(channel == index, 1.0, 0.0).astype(BF16)
            return carry

        loads[2].wait()
        lax.fori_loop(0, CHUNKS, build_hot, 0)
        loads[3].wait()
        loads[4].wait()

    with jax.named_scope("exchange_wait"):
        edge_copy().wait_recv()

        def wait_msg(step, carry):
            slot = lax.rem(pr + step, PAIR)
            msg_copy(slot, slot).wait_recv()
            return carry

        lax.fori_loop(1, PAIR, wait_msg, 0)

    with jax.named_scope("frames"):
        last = tm == TM - 1
        edge = jnp.where(last, 0.0, edge_ref[...])
        rows_ref[HOPS : HOPS + 2, :] = edge[:, :128]
        rows_ref[HOPS + 2 : HOPS + 4, :] = edge[:, 128:]

        messages = msg_ref[...].reshape(Q, 128)
        column = lax.broadcasted_iota(jnp.int32, (Q, 128), 1).astype(F32)

        def samples(part, half, ahead):
            return rows_ref[pl.ds(2 * half + part + 4 * ahead, Q, stride=4), :]

        for u in range(4):
            start = messages[:, u : u + 1]
            cosine = messages[:, 4 + u : 5 + u]
            sine = messages[:, 8 + u : 9 + u]
            halves = []
            for half in range(2):
                lanes = slice(128 * half, 128 * half + 128)
                weight = win_ref[0:1, lanes] + cosine * win_ref[1:2, lanes] + sine * win_ref[2:3, lanes]
                here = column + 128.0 * half >= start
                halves.append(
                    [jnp.where(here, samples(part, half, 0), samples(part, half, 1)) * weight for part in range(2)]
                )
            for sign in range(2):
                for part in range(2):
                    left, right = halves[0][part], halves[1][part]
                    high, low = high_low(left - right if sign else left + right)
                    grid_ref[sign, 0, u * Q : (u + 1) * Q, 128 * part : 128 * (part + 1)] = high
                    grid_ref[sign, 1, u * Q : (u + 1) * Q, 128 * part : 128 * (part + 1)] = low

    with jax.named_scope("spectra"):
        for odd in range(2):
            high, low = grid_ref[odd, 0], grid_ref[odd, 1]
            result = dot(high, tab_ref[2 * odd]) + dot(low, tab_ref[2 * odd]) + dot(high, tab_ref[2 * odd + 1])
            high, low = high_low(result)
            for u in range(4):
                for block in range(BLOCKS):
                    source = slice(u * Q + 16 * block, u * Q + 16 * block + 16)
                    for part in range(2):
                        target = slice(block * 128 + part * 64 + 16 * u, block * 128 + part * 64 + 16 * u + 16)
                        lanes = slice(128 * part, 128 * part + 128)
                        spec_ref[target, 128 * odd : 128 * odd + 128] = high[source, lanes]
                        spec_ref[target, 256 + 128 * odd : 384 + 128 * odd] = low[source, lanes]

    with jax.named_scope("main"):
        def part_copy(slot, owner):
            return pltpu.make_async_remote_copy(
                src_ref=part_ref.at[owner],
                dst_ref=recv_ref.at[slot],
                send_sem=part_send.at[owner],
                recv_sem=part_recv.at[slot],
                device_id=(owner, pr),
                device_id_type=MESH,
            )

        def compute(step, carry):
            chunk = lax.rem(tm // 2 + 1 + step, CHUNKS)
            pick_a = hot_ref[chunk, 0]
            pick_b = hot_ref[chunk, 1]
            first = dot(spec_ref[:, :NP], pick_a) + dot(spec_ref[:, NP:], pick_a)
            second = dot(spec_ref[:, :NP], pick_b) + dot(spec_ref[:, NP:], pick_b)
            power = jnp.zeros((Q, WIDTH), F32)
            for block in range(BLOCKS):
                base = block * 2 * Q
                first_re, first_im = first[base : base + Q], first[base + Q : base + 2 * Q]
                second_re, second_im = second[base : base + Q], second[base + Q : base + 2 * Q]
                re_high, re_low = high_low(first_re * second_re + first_im * second_im)
                im_high, im_low = high_low(first_im * second_re - first_re * second_im)
                stacked = jnp.concatenate([re_high, im_high, re_low, im_low], axis=0)
                both = dot(tab_ref[4], stacked)
                cyclic = both[: 2 * Q] + both[2 * Q :]
                square = cyclic * cyclic
                power = power + square[:Q] + square[Q:]
            for half in range(2):
                owner = 2 * chunk + half
                part_ref[owner] = power[:, half * SLICE : (half + 1) * SLICE]

                @pl.when(owner != tm)
                def send():
                    part_copy(tm, owner).start()

            return carry

        lax.fori_loop(0, CHUNKS, compute, 0)

    with jax.named_scope("absorb"):
        def absorb(step, total):
            slot = lax.rem(tm + step, TM)
            part_copy(slot, slot).wait_recv()
            return total + recv_ref[slot]

        total = lax.fori_loop(1, TM, absorb, part_ref[tm])
        done_ref[tm] = total * (1.0 / Q)

    with jax.named_scope("gather_send"):
        def done_copy(slot, peer):
            return pltpu.make_async_remote_copy(
                src_ref=done_ref.at[slot],
                dst_ref=done_ref.at[slot],
                send_sem=done_send.at[peer],
                recv_sem=done_recv.at[slot],
                device_id=(peer, pr),
                device_id_type=MESH,
            )

        def send_done(step, carry):
            done_copy(tm, lax.rem(tm + step, TM)).start()
            return carry

        lax.fori_loop(1, TM, send_done, 0)

    with jax.named_scope("gather_wait"):
        def wait_done(step, carry):
            slot = lax.rem(tm + step, TM)
            done_copy(slot, slot).wait_recv()
            return carry

        lax.fori_loop(1, TM, wait_done, 0)

    with jax.named_scope("output"):
        for slot in range(TM):
            out_ref[:, SLICE * slot : SLICE * (slot + 1)] = done_ref[slot]

    with jax.named_scope("drain"):
        edge_copy().wait_send()

        def drain_msg(step, carry):
            msg_copy(pr, lax.rem(pr + step, PAIR)).wait_send()
            return carry

        def drain_tm(step, carry):
            peer = lax.rem(tm + step, TM)
            part_copy(tm, peer).wait_send()
            done_copy(tm, peer).wait_send()
            return carry

        lax.fori_loop(1, PAIR, drain_msg, 0)
        lax.fori_loop(1, TM, drain_tm, 0)


def shards(signal, hop_offsets, pair_channels):
    vmem = pl.BlockSpec(memory_space=pltpu.VMEM)
    return pl.pallas_call(
        kernel,
        out_shape=jax.ShapeDtypeStruct((Q, PAIRS), F32),
        in_specs=[pl.BlockSpec(memory_space=pltpu.HBM)] * 5,
        out_specs=vmem,
        scratch_shapes=[
            pltpu.VMEM((2, HOPS * Q), F32),
            pltpu.VMEM((1, HOPS // PAIR), jnp.int32),
            pltpu.VMEM((2, PAIRS), jnp.int32),
            pltpu.VMEM((8, NP), F32),
            pltpu.VMEM((HOPS + 8, 128), F32),
            pltpu.VMEM((2, NP), F32),
            pltpu.VMEM((PAIR, 8, 128), F32),
            pltpu.VMEM((5, NP, NP), BF16),
            pltpu.VMEM((2, 2, HOPS, NP), BF16),
            pltpu.VMEM((2 * HOPS, 2 * NP), BF16),
            pltpu.VMEM((CHUNKS, 2, NP, WIDTH), BF16),
            pltpu.VMEM((TM, Q, SLICE), F32),
            pltpu.VMEM((TM, Q, SLICE), F32),
            pltpu.VMEM((TM, Q, SLICE), F32),
            pltpu.SemaphoreType.DMA((5,)),
            pltpu.SemaphoreType.DMA,
            pltpu.SemaphoreType.DMA,
            pltpu.SemaphoreType.DMA((PAIR,)),
            pltpu.SemaphoreType.DMA((PAIR,)),
            pltpu.SemaphoreType.DMA((TM,)),
            pltpu.SemaphoreType.DMA((TM,)),
            pltpu.SemaphoreType.DMA((TM,)),
            pltpu.SemaphoreType.DMA((TM,)),
        ],
        compiler_params=pltpu.CompilerParams(
            collective_id=0, has_side_effects=True, vmem_limit_bytes=48 * 1024 * 1024
        ),
    )(
        *(
            pltpu.with_memory_space_constraint(operand, pltpu.HBM)
            for operand in (
                signal,
                hop_offsets.reshape(1, HOPS // PAIR),
                pair_channels,
                jnp.asarray(window_rows()),
                jnp.asarray(tables()),
            )
        )
    )


def solution(mesh):
    return jax.shard_map(
        shards,
        mesh=mesh,
        in_specs=(P(None, "tm"), P(("tm", "pair")), P(None, "pair")),
        out_specs=P(None, "pair"),
        check_vma=False,
    )
```

```python
import numpy as np

import jax
import jax.numpy as jnp
from jax import lax
from jax.experimental import pallas as pl
from jax.experimental.pallas import tpu as pltpu
from jax.sharding import PartitionSpec as P

NP = 256
Q = 64
TM = 16
PAIR = 8
HOPS = 256
PAIRS = 2048
WIDTH = 256
CHUNKS = PAIRS // WIDTH
GROUPS = CHUNKS // 2
BLOCKS = HOPS // Q
MESH = pl.DeviceIdType.MESH
F32 = jnp.float32
BF16 = jnp.bfloat16


def split(table):
    high = table.astype(np.float32).astype(BF16)
    low = (table - high.astype(np.float64)).astype(np.float32).astype(BF16)
    return high, low


def tables():
    sample = np.arange(NP // 2)
    out = []
    for odd in (0, 1):
        turns = np.outer(sample, 2 * sample + odd) % NP
        angle = 2.0 * np.pi * turns / NP
        cosine, sine = np.cos(angle), np.sin(angle)
        table = np.block([[cosine, -sine], [sine, cosine]])
        out.extend(split(table))
    hop = (4 * np.arange(Q // 4)[None, :] + np.arange(4)[:, None]).reshape(Q)
    turns = np.outer(np.arange(Q), hop) % Q
    angle = 2.0 * np.pi * turns / Q
    cosine, sine = np.cos(angle) / 8.0, np.sin(angle) / 8.0
    high, low = split(np.block([[cosine, sine], [-sine, cosine]]))
    upper = np.concatenate([high, high], axis=1)
    lower = np.concatenate([low, np.zeros_like(low)], axis=1)
    out.append(np.concatenate([upper, lower], axis=0))
    return np.stack(out)


def window_rows():
    sample = np.arange(NP)
    angle = 2.0 * np.pi * sample / NP
    window = 0.54 - 0.46 * np.cos(angle)
    gain = 1.0 / np.sqrt(np.sum(window * window))
    rows = np.zeros((8, NP))
    rows[0] = 0.54 * gain
    rows[1] = -0.46 * gain * np.cos(angle)
    rows[2] = -0.46 * gain * np.sin(angle)
    return rows.astype(np.float32)


def high_low(value):
    high = value.astype(BF16)
    return high, (value - high.astype(F32)).astype(BF16)


def dot(left, right):
    return jnp.dot(left, right, preferred_element_type=F32)


def ring(distance, size):
    return min(distance, size - distance)


TM_STEPS = sorted(
    ((dz, dx) for dz in range(4) for dx in range(4) if dz or dx),
    key=lambda step: -(ring(step[0], 4) + ring(step[1], 4)),
)
PAIR_STEPS = sorted(
    ((dy, dc) for dy in range(4) for dc in range(2) if dy or dc),
    key=lambda step: -(2 * ring(step[0], 4) + step[1]),
)


def tm_peer(tm, step, sign=1):
    dz, dx = step
    return ((tm // 4 + sign * dz) % 4) * 4 + (tm % 4 + sign * dx) % 4


def pair_peer(pr, step, sign=1):
    dy, dc = step
    return ((pr // 2 + sign * dy) % 4) * 2 + (pr % 2 + dc) % 2


def exchange_kernel(
    sig_hbm, off_hbm, pc_hbm, win_hbm, tab_hbm,
    rows_ref, msg_ref, hot_ref, tab_ref, win_ref,
    sig_ref, off_ref, pc_ref, edge_ref,
    load_sem, edge_send, edge_recv, msg_send, msg_recv,
):
    tm = lax.axis_index("tm")
    pr = lax.axis_index("pair")
    before = (tm + TM - 1) % TM
    after = (tm + 1) % TM

    with jax.named_scope("load_greet"):
        barrier = pltpu.get_barrier_semaphore()
        for near, peer in ((tm > 0, before), (tm < TM - 1, after)):

            @pl.when(near)
            def greet():
                pl.semaphore_signal(barrier, inc=1, device_id=(peer, pr), device_id_type=MESH)

        for step in PAIR_STEPS:
            pl.semaphore_signal(barrier, inc=1, device_id=(tm, pair_peer(pr, step)), device_id_type=MESH)
        loads = [
            pltpu.make_async_copy(source, target, load_sem.at[index])
            for index, (source, target) in enumerate(
                (
                    (off_hbm, off_ref),
                    (sig_hbm, sig_ref),
                    (pc_hbm, pc_ref),
                    (win_hbm, win_ref),
                    (tab_hbm, tab_ref),
                )
            )
        ]
        for load in loads:
            load.start()

    with jax.named_scope("prep"):
        loads[0].wait()
        lane = lax.broadcasted_iota(jnp.int32, (8, 128), 1)
        row32 = lax.broadcasted_iota(jnp.int32, (8, 32), 0)
        lane32 = lax.broadcasted_iota(jnp.int32, (8, 32), 1)
        shift = (off_ref[...] & (NP - 1)).astype(F32)
        shift = jnp.broadcast_to(shift, (8, 32))
        value = jnp.zeros((8, 128), F32)
        for u in range(4):
            column = jnp.sum(jnp.where(lane32 == 4 * row32 + u, shift, 0.0), axis=1, keepdims=True)
            value = jnp.where((lane & 3) == u, column, value)
        theta = value * (2.0 * np.pi / NP)
        value = jnp.where(lane < 4, value, jnp.where(lane < 8, jnp.cos(theta), jnp.sin(theta)))
        msg_ref[pr] = value
        loads[1].wait()

    with jax.named_scope("barrier"):
        ends = jnp.where((tm == 0) | (tm == TM - 1), 1, 2)
        pl.semaphore_wait(barrier, PAIR - 1 + ends)

    with jax.named_scope("exchange_start"):
        def msg_copy(index, slot):
            return pltpu.make_async_remote_copy(
                src_ref=msg_ref.at[slot],
                dst_ref=msg_ref.at[slot],
                send_sem=msg_send,
                recv_sem=msg_recv,
                device_id=(tm, pair_peer(pr, PAIR_STEPS[index])),
                device_id_type=MESH,
            )

        edge_copy = pltpu.make_async_remote_copy(
            src_ref=sig_ref.at[:, pl.ds(0, NP)],
            dst_ref=edge_ref,
            send_sem=edge_send,
            recv_sem=edge_recv,
            device_id=(before, pr),
            device_id_type=MESH,
        )
        for index in range(PAIR - 1):
            msg_copy(index, pr).start()

        @pl.when(tm > 0)
        def send_edge():
            edge_copy.start()


    with jax.named_scope("hot"):
        for group in range(HOPS // 2):
            rows_ref[2 * group : 2 * group + 2, :] = sig_ref[:, 128 * group : 128 * (group + 1)]

        channel = lax.broadcasted_iota(jnp.int32, (NP, WIDTH), 0)

        def build_hot(chunk, carry):
            start = pl.multiple_of(chunk * WIDTH, WIDTH)
            for side in range(2):
                index = pc_ref[side : side + 1, pl.ds(start, WIDTH)]
                index = (index >> 1) + (index & 1) * (NP // 2)
                hot_ref[chunk, side] = jnp.where(channel == index, 1.0, 0.0).astype(BF16)
            return carry

        loads[2].wait()
        lax.fori_loop(0, CHUNKS, build_hot, 0)
        loads[3].wait()
        loads[4].wait()

    with jax.named_scope("exchange_wait"):
        others = msg_ref.at[pl.ds(0, PAIR - 1)]
        arrived = pltpu.make_async_remote_copy(
            src_ref=others,
            dst_ref=others,
            send_sem=msg_send,
            recv_sem=msg_recv,
            device_id=(tm, pair_peer(pr, PAIR_STEPS[0])),
            device_id_type=MESH,
        )
        rows_ref[HOPS : HOPS + 8, :] = jnp.zeros((8, 128), F32)

        @pl.when(tm < TM - 1)
        def take_edge():
            edge_copy.wait_recv()
            rows_ref[HOPS : HOPS + 2, :] = edge_ref[:, :128]
            rows_ref[HOPS + 2 : HOPS + 4, :] = edge_ref[:, 128:]

        arrived.wait_recv()
        arrived.wait_send()

        @pl.when(tm > 0)
        def edge_left():
            edge_copy.wait_send()


def main_kernel(
    rows_ref, msg_ref, hot_ref, tab_ref, win_ref, out_ref,
    grid_ref, spec_ref, part_ref, recv_ref,
    part_send, part_recv, done_send, done_recv,
):
    tm = lax.axis_index("tm")
    pr = lax.axis_index("pair")
    with jax.named_scope("greet"):
        barrier = pltpu.get_barrier_semaphore()
        peers = [tm_peer(tm, step) for step in TM_STEPS]
        for peer in peers:
            pl.semaphore_signal(barrier, inc=1, device_id=(peer, pr), device_id_type=MESH)

    with jax.named_scope("frames"):
        messages = msg_ref[...].reshape(Q, 128)
        column = lax.broadcasted_iota(jnp.int32, (Q, 128), 1).astype(F32)

        def samples(part, half, ahead):
            return rows_ref[pl.ds(2 * half + part + 4 * ahead, Q, stride=4), :]

        for u in range(4):
            start = messages[:, u : u + 1]
            cosine = messages[:, 4 + u : 5 + u]
            sine = messages[:, 8 + u : 9 + u]
            halves = []
            for half in range(2):
                lanes = slice(128 * half, 128 * half + 128)
                weight = win_ref[0:1, lanes] + cosine * win_ref[1:2, lanes] + sine * win_ref[2:3, lanes]
                here = column + 128.0 * half >= start
                halves.append(
                    [jnp.where(here, samples(part, half, 0), samples(part, half, 1)) * weight for part in range(2)]
                )
            for sign in range(2):
                for part in range(2):
                    left, right = halves[0][part], halves[1][part]
                    high, low = high_low(left - right if sign else left + right)
                    grid_ref[sign, 0, u * Q : (u + 1) * Q, 128 * part : 128 * (part + 1)] = high
                    grid_ref[sign, 1, u * Q : (u + 1) * Q, 128 * part : 128 * (part + 1)] = low

    with jax.named_scope("spectra"):
        for odd in range(2):
            high, low = grid_ref[odd, 0], grid_ref[odd, 1]
            result = dot(high, tab_ref[2 * odd]) + dot(low, tab_ref[2 * odd]) + dot(high, tab_ref[2 * odd + 1])
            high, low = high_low(result)
            for u in range(4):
                for block in range(BLOCKS):
                    source = slice(u * Q + 16 * block, u * Q + 16 * block + 16)
                    for part in range(2):
                        target = slice(block * 128 + part * 64 + 16 * u, block * 128 + part * 64 + 16 * u + 16)
                        lanes = slice(128 * part, 128 * part + 128)
                        spec_ref[target, 128 * odd : 128 * odd + 128] = high[source, lanes]
                        spec_ref[target, 256 + 128 * odd : 384 + 128 * odd] = low[source, lanes]

    def part_copy(group, index):
        return pltpu.make_async_remote_copy(
            src_ref=part_ref.at[group, peers[index]],
            dst_ref=recv_ref.at[group, index],
            send_sem=part_send,
            recv_sem=part_recv.at[group],
            device_id=(peers[index], pr),
            device_id_type=MESH,
        )

    def slice_of(group, owner):
        rows = pl.ds(pl.multiple_of(8 * (owner % 8), 8), 8)
        return rows, pl.ds(pl.multiple_of(WIDTH * (2 * group + owner // 8), WIDTH), WIDTH)

    def done_copy(group, index, owner):
        rows, lanes = slice_of(group, owner)
        return pltpu.make_async_remote_copy(
            src_ref=out_ref.at[rows, lanes],
            dst_ref=out_ref.at[rows, lanes],
            send_sem=done_send,
            recv_sem=done_recv,
            device_id=(peers[index], pr),
            device_id_type=MESH,
        )

    with jax.named_scope("main"):
        def pick(chunk):
            return [
                dot(spec_ref[:, :NP], hot_ref[chunk, side]) + dot(spec_ref[:, NP:], hot_ref[chunk, side])
                for side in range(2)
            ]

        def power_of(first, second):
            power = None
            for block in range(BLOCKS):
                base = block * 2 * Q
                first_re, first_im = first[base : base + Q], first[base + Q : base + 2 * Q]
                second_re, second_im = second[base : base + Q], second[base + Q : base + 2 * Q]
                re_high, re_low = high_low(first_re * second_re + first_im * second_im)
                im_high, im_low = high_low(first_im * second_re - first_re * second_im)
                stacked = jnp.concatenate([re_high, im_high, re_low, im_low], axis=0)
                both = dot(tab_ref[4], stacked)
                cyclic = both[: 2 * Q] + both[2 * Q :]
                square = cyclic * cyclic
                square = square[:Q] + square[Q:]
                power = square if power is None else power + square
            return power

        for chunk in range(CHUNKS):
            power = power_of(*pick(chunk))
            group, side = chunk // 2, chunk % 2
            for row in range(8):
                part_ref[group, 8 * side + row] = power[8 * row : 8 * row + 8]
            if side:
                if group == 0:
                    pl.semaphore_wait(barrier, TM - 1)
                for index in range(TM - 1):
                    part_copy(group, index).start()

    def all_of(target, send_sem, recv_sem):
        return pltpu.make_async_remote_copy(
            src_ref=target,
            dst_ref=target,
            send_sem=send_sem,
            recv_sem=recv_sem,
            device_id=(peers[0], pr),
            device_id_type=MESH,
        )

    for group in range(GROUPS):
        with jax.named_scope("absorb"):
            all_of(recv_ref.at[group], part_send, part_recv.at[group]).wait_recv()
            total = part_ref[group, tm]
            for index in range(TM - 1):
                total = total + recv_ref[group, index]
            rows, lanes = slice_of(group, tm)
            out_ref[rows, lanes] = total * (1.0 / Q)
            for index in range(TM - 1):
                done_copy(group, index, tm).start()

    with jax.named_scope("gather_wait"):
        all_done = all_of(recv_ref, done_send, done_recv)
        all_done.wait_recv()

    with jax.named_scope("drain"):
        all_of(recv_ref, part_send, done_recv).wait_send()
        all_done.wait_send()


def in_hbm(array):
    return pltpu.with_memory_space_constraint(array, pltpu.HBM)


def in_vmem(array):
    return pltpu.with_memory_space_constraint(array, pltpu.VMEM)


def shards(signal, hop_offsets, pair_channels):
    vmem = pl.BlockSpec(memory_space=pltpu.VMEM)
    hbm = pl.BlockSpec(memory_space=pltpu.HBM)
    passed = (
        ((HOPS + 8, 128), F32),
        ((PAIR, 8, 128), F32),
        ((CHUNKS, 2, NP, WIDTH), BF16),
        ((5, NP, NP), BF16),
        ((8, NP), F32),
    )
    staged = pl.pallas_call(
        exchange_kernel,
        out_shape=[pltpu.VMEM(*shape) for shape in passed],
        in_specs=[hbm] * 5,
        out_specs=[vmem] * 5,
        scratch_shapes=[
            pltpu.VMEM((2, HOPS * Q), F32),
            pltpu.VMEM((1, HOPS // PAIR), jnp.int32),
            pltpu.VMEM((2, PAIRS), jnp.int32),
            pltpu.VMEM((2, NP), F32),
            pltpu.SemaphoreType.DMA((5,)),
            pltpu.SemaphoreType.DMA,
            pltpu.SemaphoreType.DMA,
            pltpu.SemaphoreType.DMA,
            pltpu.SemaphoreType.DMA,
        ],
        compiler_params=pltpu.CompilerParams(
            collective_id=0, has_side_effects=True, vmem_limit_bytes=16 * 1024 * 1024
        ),
    )(
        in_hbm(signal),
        in_hbm(hop_offsets.reshape(1, HOPS // PAIR)),
        in_hbm(pair_channels),
        in_hbm(jnp.asarray(window_rows())),
        in_hbm(jnp.asarray(tables())),
    )
    return pl.pallas_call(
        main_kernel,
        out_shape=jax.ShapeDtypeStruct((Q, PAIRS), F32),
        in_specs=[vmem] * 5,
        out_specs=vmem,
        scratch_shapes=[
            pltpu.VMEM((2, 2, HOPS, NP), BF16),
            pltpu.VMEM((2 * HOPS, 2 * NP), BF16),
            pltpu.VMEM((GROUPS, TM, 8, WIDTH), F32),
            pltpu.VMEM((GROUPS, TM - 1, 8, WIDTH), F32),
            pltpu.SemaphoreType.DMA,
            pltpu.SemaphoreType.DMA((GROUPS,)),
            pltpu.SemaphoreType.DMA,
            pltpu.SemaphoreType.DMA,
        ],
        compiler_params=pltpu.CompilerParams(
            collective_id=1, has_side_effects=True, vmem_limit_bytes=32 * 1024 * 1024
        ),
    )(*(in_vmem(array) for array in staged))


def solution(mesh):
    return jax.shard_map(
        shards,
        mesh=mesh,
        in_specs=(P(None, "tm"), P(("tm", "pair")), P(None, "pair")),
        out_specs=P(None, "pair"),
        check_vma=False,
    )
```

```python
import numpy as np

import jax
import jax.numpy as jnp
from jax import lax
from jax.experimental import pallas as pl
from jax.experimental.pallas import tpu as pltpu
from jax.sharding import PartitionSpec as P

NP = 256
Q = 64
TM = 16
PAIR = 8
HOPS = 256
PAIRS = 2048
WIDTH = 256
CHUNKS = PAIRS // WIDTH
STAGED = ((0, 2), (2, 4), (4, 6), (6, 8))
STAGED_CHUNKS = STAGED[-1][1]
ORDER = tuple((name, group) for name in ("first", "second") for group in range(len(STAGED)))
BLOCKS = HOPS // Q
MESH = pl.DeviceIdType.MESH
F32 = jnp.float32
BF16 = jnp.bfloat16


def split(table):
    high = table.astype(np.float32).astype(BF16)
    low = (table - high.astype(np.float64)).astype(np.float32).astype(BF16)
    return high, low


def tables():
    sample = np.arange(NP // 2)
    out = []
    for odd in (0, 1):
        turns = np.outer(sample, 2 * sample + odd) % NP
        angle = 2.0 * np.pi * turns / NP
        cosine, sine = np.cos(angle), np.sin(angle)
        table = np.block([[cosine, -sine], [sine, cosine]])
        out.extend(split(table))
    hop = (4 * np.arange(Q // 4)[None, :] + np.arange(4)[:, None]).reshape(Q)
    turns = np.outer(np.arange(Q), hop) % Q
    angle = 2.0 * np.pi * turns / Q
    cosine, sine = np.cos(angle) / 8.0, np.sin(angle) / 8.0
    high, low = split(np.block([[cosine, sine], [-sine, cosine]]))
    upper = np.concatenate([high, high], axis=1)
    lower = np.concatenate([low, np.zeros_like(low)], axis=1)
    out.append(np.concatenate([upper, lower], axis=0))
    return np.stack(out)


def window_rows():
    sample = np.arange(NP)
    angle = 2.0 * np.pi * sample / NP
    window = 0.54 - 0.46 * np.cos(angle)
    gain = 1.0 / np.sqrt(np.sum(window * window))
    rows = np.zeros((8, NP))
    rows[0] = 0.54 * gain
    rows[1] = -0.46 * gain * np.cos(angle)
    rows[2] = -0.46 * gain * np.sin(angle)
    return rows.astype(np.float32)


def high_low(value):
    high = value.astype(BF16)
    return high, (value - high.astype(F32)).astype(BF16)


def dot(left, right):
    return jnp.dot(left, right, preferred_element_type=F32)


def ring(distance, size):
    return min(distance, size - distance)


TM_STEPS = sorted(
    ((dz, dx) for dz in range(4) for dx in range(4) if dz or dx),
    key=lambda step: -(ring(step[0], 4) + ring(step[1], 4)),
)
PAIR_STEPS = sorted(
    ((dy, dc) for dy in range(4) for dc in range(2) if dy or dc),
    key=lambda step: -(2 * ring(step[0], 4) + step[1]),
)


def tm_peer(tm, step, sign=1):
    dz, dx = step
    return ((tm // 4 + sign * dz) % 4) * 4 + (tm % 4 + sign * dx) % 4


def pair_peer(pr, step, sign=1):
    dy, dc = step
    return ((pr // 2 + sign * dy) % 4) * 2 + (pr % 2 + dc) % 2


def kernel(
    sig_hbm, off_hbm, pc_hbm, win_hbm, tab_hbm, out_ref,
    sig_ref, off_ref, pc_ref, win_ref, tab_ref, rows_ref, edge_ref, msg_ref, hot_ref,
    grid_ref, spec_ref, pair_ref, part_ref, first_ref, mid_ref, done_ref,
    load_sem, ready_sem, edge_send, edge_recv, msg_send, msg_recv,
    stage_send, stage_recv,
):
    tm = lax.axis_index("tm")
    pr = lax.axis_index("pair")
    before = (tm + TM - 1) % TM
    after = (tm + 1) % TM
    peers = [tm_peer(tm, step) for step in TM_STEPS]
    in_row = [peer for peer, (dz, dx) in zip(peers, TM_STEPS) if dz == 0]
    tm_row, tm_column = tm // 4, tm % 4
    far_before = (tm_column == 0) & (tm_row > 0)
    far_after = (tm_column == 3) & (tm_row < 3)

    def signal(semaphore, peer):
        pl.semaphore_signal(semaphore, inc=1, device_id=(peer, pr), device_id_type=MESH)

    def signal_column(semaphore, first, last):
        lax.fori_loop(first, last, lambda z, carry: signal(semaphore, 4 * z + tm_column), None)

    def signal_row(semaphore, first, last):
        lax.fori_loop(first, last, lambda x, carry: signal(semaphore, 4 * tm_row + x), None)

    with jax.named_scope("load_greet"):
        barrier = pltpu.get_barrier_semaphore()
        for step in PAIR_STEPS:
            pl.semaphore_signal(barrier, inc=1, device_id=(tm, pair_peer(pr, step)), device_id_type=MESH)
        signal_column(barrier, tm_row + 1, jnp.int32(4))
        signal_row(barrier, tm_column + 1, jnp.int32(4))

        @pl.when(far_after)
        def greet():
            signal(barrier, after)

        loads = [
            pltpu.make_async_copy(source, target, load_sem.at[index])
            for index, (source, target) in enumerate(
                (
                    (off_hbm, off_ref),
                    (sig_hbm, sig_ref),
                    (pc_hbm, pc_ref),
                    (win_hbm, win_ref),
                    (tab_hbm, tab_ref),
                )
            )
        ]
        for load in loads:
            load.start()

    with jax.named_scope("prep"):
        loads[0].wait()
        lane = lax.broadcasted_iota(jnp.int32, (8, 128), 1)
        row32 = lax.broadcasted_iota(jnp.int32, (8, 32), 0)
        lane32 = lax.broadcasted_iota(jnp.int32, (8, 32), 1)
        shift = (off_ref[...] & (NP - 1)).astype(F32)
        shift = jnp.broadcast_to(shift, (8, 32))
        value = jnp.zeros((8, 128), F32)
        for u in range(4):
            column = jnp.sum(jnp.where(lane32 == 4 * row32 + u, shift, 0.0), axis=1, keepdims=True)
            value = jnp.where((lane & 3) == u, column, value)
        theta = value * (2.0 * np.pi / NP)
        value = jnp.where(lane < 4, value, jnp.where(lane < 8, jnp.cos(theta), jnp.sin(theta)))
        msg_ref[pr] = value
        loads[1].wait()

    with jax.named_scope("barrier"):
        pl.semaphore_wait(barrier, PAIR - 1 + tm_row + tm_column + jnp.where(far_before, 1, 0))

    with jax.named_scope("exchange_start"):
        def msg_copy(index, slot):
            return pltpu.make_async_remote_copy(
                src_ref=msg_ref.at[slot],
                dst_ref=msg_ref.at[slot],
                send_sem=msg_send,
                recv_sem=msg_recv,
                device_id=(tm, pair_peer(pr, PAIR_STEPS[index])),
                device_id_type=MESH,
            )

        edge_copy = pltpu.make_async_remote_copy(
            src_ref=sig_ref.at[:, pl.ds(0, NP)],
            dst_ref=edge_ref,
            send_sem=edge_send,
            recv_sem=edge_recv,
            device_id=(before, pr),
            device_id_type=MESH,
        )
        for index in range(PAIR - 1):
            msg_copy(index, pr).start()

        @pl.when(tm > 0)
        def send_edge():
            edge_copy.start()

        signal_column(ready_sem, jnp.int32(0), tm_row)
        signal_row(ready_sem, jnp.int32(0), tm_column)

    with jax.named_scope("hot"):
        for group in range(HOPS // 2):
            rows_ref[2 * group : 2 * group + 2, :] = sig_ref[:, 128 * group : 128 * (group + 1)]

        channel = lax.broadcasted_iota(jnp.int32, (NP, WIDTH), 0)

        def build_hot(chunk, carry):
            start = pl.multiple_of(chunk * WIDTH, WIDTH)
            for side in range(2):
                index = pc_ref[side : side + 1, pl.ds(start, WIDTH)]
                index = (index >> 1) + (index & 1) * (NP // 2)
                hot_ref[chunk, side] = jnp.where(channel == index, 1.0, 0.0).astype(BF16)
            return carry

        loads[2].wait()
        lax.fori_loop(0, CHUNKS, build_hot, 0)
        loads[3].wait()
        loads[4].wait()

    with jax.named_scope("ready"):
        @pl.when(tm < TM - 1)
        def wait_ready():
            pl.semaphore_wait(ready_sem, 6 - tm_row - tm_column)

    with jax.named_scope("exchange_wait"):
        others = msg_ref.at[pl.ds(0, PAIR - 1)]
        arrived = pltpu.make_async_remote_copy(
            src_ref=others,
            dst_ref=others,
            send_sem=msg_send,
            recv_sem=msg_recv,
            device_id=(tm, pair_peer(pr, PAIR_STEPS[0])),
            device_id_type=MESH,
        )
        rows_ref[HOPS : HOPS + 8, :] = jnp.zeros((8, 128), F32)

        @pl.when(tm < TM - 1)
        def take_edge():
            edge_copy.wait_recv()
            rows_ref[HOPS : HOPS + 2, :] = edge_ref[:, :128]
            rows_ref[HOPS + 2 : HOPS + 4, :] = edge_ref[:, 128:]

        arrived.wait_recv()
        arrived.wait_send()

        @pl.when(tm > 0)
        def edge_left():
            edge_copy.wait_send()

    with jax.named_scope("frames"):
        messages = msg_ref[...].reshape(Q, 128)
        column = lax.broadcasted_iota(jnp.int32, (Q, 128), 1).astype(F32)

        def samples(part, half, ahead):
            return rows_ref[pl.ds(2 * half + part + 4 * ahead, Q, stride=4), :]

        for u in range(4):
            start = messages[:, u : u + 1]
            cosine = messages[:, 4 + u : 5 + u]
            sine = messages[:, 8 + u : 9 + u]
            halves = []
            for half in range(2):
                lanes = slice(128 * half, 128 * half + 128)
                weight = win_ref[0:1, lanes] + cosine * win_ref[1:2, lanes] + sine * win_ref[2:3, lanes]
                here = column + 128.0 * half >= start
                halves.append(
                    [jnp.where(here, samples(part, half, 0), samples(part, half, 1)) * weight for part in range(2)]
                )
            for sign in range(2):
                for part in range(2):
                    left, right = halves[0][part], halves[1][part]
                    high, low = high_low(left - right if sign else left + right)
                    grid_ref[sign, 0, u * Q : (u + 1) * Q, 128 * part : 128 * (part + 1)] = high
                    grid_ref[sign, 1, u * Q : (u + 1) * Q, 128 * part : 128 * (part + 1)] = low

    with jax.named_scope("spectra"):
        for odd in range(2):
            high, low = grid_ref[odd, 0], grid_ref[odd, 1]
            result = dot(high, tab_ref[2 * odd]) + dot(low, tab_ref[2 * odd]) + dot(high, tab_ref[2 * odd + 1])
            high, low = high_low(result)
            for u in range(4):
                for block in range(BLOCKS):
                    source = slice(u * Q + 16 * block, u * Q + 16 * block + 16)
                    for part in range(2):
                        target = slice(block * 128 + part * 64 + 16 * u, block * 128 + part * 64 + 16 * u + 16)
                        lanes = slice(128 * part, 128 * part + 128)
                        spec_ref[target, 128 * odd : 128 * odd + 128] = high[source, lanes]
                        spec_ref[target, 256 + 128 * odd : 384 + 128 * odd] = low[source, lanes]

    def stage_copy(group, chunk, stage, step):
        even = chunk % 2 == 0
        mine, other = (tm_column, tm_row) if even else (tm_row, tm_column)
        if even == (stage != 1):
            peer = 4 * tm_row + (tm_column + step) % 4
        else:
            peer = 4 * ((tm_row + step) % 4) + tm_column
        if stage == 0:
            source, target = part_ref.at[chunk, (mine + step) % 4], first_ref.at[chunk, step - 1]
        elif stage == 1:
            source = target = mid_ref.at[chunk, other]
        else:
            source = target = done_ref.at[chunk, mine]
        return pltpu.make_async_remote_copy(
            src_ref=source,
            dst_ref=target,
            send_sem=stage_send.at[stage],
            recv_sem=stage_recv.at[3 * group + stage],
            device_id=(peer, pr),
            device_id_type=MESH,
        )

    def send_stage(group, stage):
        for step in (2, 1, 3):
            for chunk in range(*STAGED[group]):
                stage_copy(group, chunk, stage, step).start()

    def all_of(target, send_sem, recv_sem):
        return pltpu.make_async_remote_copy(
            src_ref=target,
            dst_ref=target,
            send_sem=send_sem,
            recv_sem=recv_sem,
            device_id=(peers[0], pr),
            device_id_type=MESH,
        )

    def wait_stage(group, stage):
        first, last = STAGED[group]
        target = first_ref.at[pl.ds(first, last - first)]
        all_of(target, stage_send.at[stage], stage_recv.at[3 * group + stage]).wait_recv()

    with jax.named_scope("main"):
        def pick(chunk):
            for side in range(2):
                pair_ref[chunk % 2, side] = dot(spec_ref[:, :NP], hot_ref[chunk, side]) + dot(
                    spec_ref[:, NP:], hot_ref[chunk, side]
                )

        def power_of(slot):
            power = None
            for block in range(BLOCKS):
                base = block * 2 * Q
                first_re, first_im = (pair_ref[slot, 0, base + Q * part : base + Q * part + Q] for part in range(2))
                second_re, second_im = (pair_ref[slot, 1, base + Q * part : base + Q * part + Q] for part in range(2))
                re_high, re_low = high_low(first_re * second_re + first_im * second_im)
                im_high, im_low = high_low(first_im * second_re - first_re * second_im)
                stacked = jnp.concatenate([re_high, im_high, re_low, im_low], axis=0)
                both = dot(tab_ref[4], stacked)
                cyclic = both[: 2 * Q] + both[2 * Q :]
                square = cyclic * cyclic
                square = square[:Q] + square[Q:]
                power = square if power is None else power + square
            return power

        pick(0)
        staged_ends = [last for first, last in STAGED]
        for chunk in range(CHUNKS):
            if chunk + 1 < CHUNKS:
                pick(chunk + 1)
            power = power_of(chunk % 2)
            for tile in range(TM):
                rows, lanes = 8 * (tile % 8), 128 * (tile // 8)
                part_ref[chunk, tile // 4, tile % 4] = power[rows : rows + 8, lanes : lanes + 128]
            if chunk + 1 in staged_ends:
                send_stage(staged_ends.index(chunk + 1), 0)

    def sum_first(group):
        wait_stage(group, 0)
        for chunk in range(*STAGED[group]):
            mine, other = (tm_column, tm_row) if chunk % 2 == 0 else (tm_row, tm_column)
            total = part_ref[chunk, mine]
            for step in range(3):
                total = total + first_ref[chunk, step]
            mid_ref[chunk, other] = total
        send_stage(group, 1)

    def sum_second(group):
        wait_stage(group, 1)
        for chunk in range(*STAGED[group]):
            mine = tm_column if chunk % 2 == 0 else tm_row
            total = (mid_ref[chunk, 0] + mid_ref[chunk, 1]) + (mid_ref[chunk, 2] + mid_ref[chunk, 3])
            done_ref[chunk, mine] = total * (1.0 / Q)
        send_stage(group, 2)

    def put_out(chunks):
        for chunk in range(*chunks):
            for tile in range(TM):
                rows, lanes = 8 * (tile % 8), WIDTH * chunk + 128 * (tile // 8)
                out_ref[rows : rows + 8, lanes : lanes + 128] = done_ref[chunk, tile // 4, tile % 4]

    actions = {"first": sum_first, "second": sum_second}
    for name, group in ORDER:
        with jax.named_scope(f"{name}{group}"):
            actions[name](group)
    for group in range(len(STAGED)):
        with jax.named_scope(f"third{group}"):
            wait_stage(group, 2)
            put_out(STAGED[group])
    with jax.named_scope("drain"):
        for stage in range(3):
            all_of(first_ref, stage_send.at[stage], stage_recv.at[stage]).wait_send()


def in_hbm(array):
    return pltpu.with_memory_space_constraint(array, pltpu.HBM)


def shards(signal, hop_offsets, pair_channels):
    return pl.pallas_call(
        kernel,
        out_shape=jax.ShapeDtypeStruct((Q, PAIRS), F32),
        in_specs=[pl.BlockSpec(memory_space=pltpu.HBM)] * 5,
        out_specs=pl.BlockSpec(memory_space=pltpu.VMEM),
        scratch_shapes=[
            pltpu.VMEM((2, HOPS * Q), F32),
            pltpu.VMEM((1, HOPS // PAIR), jnp.int32),
            pltpu.VMEM((2, PAIRS), jnp.int32),
            pltpu.VMEM((8, NP), F32),
            pltpu.VMEM((5, NP, NP), BF16),
            pltpu.VMEM((HOPS + 8, 128), F32),
            pltpu.VMEM((2, NP), F32),
            pltpu.VMEM((PAIR, 8, 128), F32),
            pltpu.VMEM((CHUNKS, 2, NP, WIDTH), BF16),
            pltpu.VMEM((2, 2, HOPS, NP), BF16),
            pltpu.VMEM((2 * HOPS, 2 * NP), BF16),
            pltpu.VMEM((2, 2, 2 * HOPS, WIDTH), F32),
            pltpu.VMEM((CHUNKS, 4, 4, 8, 128), F32),
            pltpu.VMEM((STAGED_CHUNKS, 3, 4, 8, 128), F32),
            pltpu.VMEM((STAGED_CHUNKS, 4, 4, 8, 128), F32),
            pltpu.VMEM((CHUNKS, 4, 4, 8, 128), F32),
            pltpu.SemaphoreType.DMA((5,)),
            pltpu.SemaphoreType.REGULAR,
            pltpu.SemaphoreType.DMA,
            pltpu.SemaphoreType.DMA,
            pltpu.SemaphoreType.DMA,
            pltpu.SemaphoreType.DMA,
            pltpu.SemaphoreType.DMA((3,)),
            pltpu.SemaphoreType.DMA((3 * len(STAGED),)),
        ],
        compiler_params=pltpu.CompilerParams(
            collective_id=0, has_side_effects=True, vmem_limit_bytes=48 * 1024 * 1024
        ),
    )(
        in_hbm(signal),
        in_hbm(hop_offsets.reshape(1, HOPS // PAIR)),
        in_hbm(pair_channels),
        in_hbm(jnp.asarray(window_rows())),
        in_hbm(jnp.asarray(tables())),
    )


def solution(mesh):
    return jax.shard_map(
        shards,
        mesh=mesh,
        in_specs=(P(None, "tm"), P(("tm", "pair")), P(None, "pair")),
        out_specs=P(None, "pair"),
        check_vma=False,
    )
```
